8 devices in a mesh: dp: 1 (over z), a: 2 (over y), b: 4 (over x, core).
Axes of the slice: x: 2, y: 2, z: 1, core: 2. Of those that a mesh axis runs over, the one named last changes fastest.
Arguments:
- x: bfloat16 [2048, 12288], P('dp', ('a', 'b'))
- w_gate: bfloat16 [12288, 33792], P('a', 'b')
- w_up: bfloat16 [12288, 33792], P('a', 'b')
- w_down: bfloat16 [33792, 12288], P('b', 'a')
Outputs:
- output: bfloat16 [2048, 12288], P('dp', ('a', 'b'))
All inputs are finite; a program needn't handle non-finite values.
Results may differ from the reference program's by a relative error of at most 0.016.
Values are sent between devices in bfloat16 or wider.
A program may use at most 2 GiB of HBM per device.

```python
import jax
import jax.numpy as jnp

ROWS = 2048
D = 12288
FF = 33792


def setup_inputs(seed: int = 0, part: int = 0) -> dict:
    kx, kg, ku, kd = jax.random.split(jax.random.key(seed), 4)
    drawn = {
        "x": jax.random.normal(jax.random.fold_in(kx, part), (ROWS, D), jnp.float32),
        "w_gate": jax.random.normal(kg, (D, FF), jnp.float32) * D**-0.5,
        "w_up": jax.random.normal(ku, (D, FF), jnp.float32) * D**-0.5,
        "w_down": jax.random.normal(kd, (FF, D), jnp.float32) * FF**-0.5,
    }
    return {k: v.astype(jnp.bfloat16) for k, v in drawn.items()}


def reference(x, w_gate, w_up, w_down):
    gate = jnp.dot(x, w_gate, preferred_element_type=jnp.float32)
    up = jnp.dot(x, w_up, preferred_element_type=jnp.float32)
    hidden = (jax.nn.silu(gate) * up).astype(jnp.bfloat16)
    return jnp.dot(hidden, w_down, preferred_element_type=jnp.float32).astype(jnp.bfloat16)
```

```python
import functools
import jax
import jax.numpy as jnp
from jax import lax
from jax.experimental import pallas as pl
from jax.experimental.pallas import tpu as pltpu
from jax.sharding import PartitionSpec as P

R = 256
F = 256
GROUP = 3
LAG_HIDDEN = 4
LAG_DOWN = 12
SLOTS = LAG_DOWN + 2
HSLOTS = LAG_DOWN // GROUP + 1
WSLOTS = 2
VMEM_LIMIT = 66 * 1000 * 1000


def kernel(x, w_gate, w_up, w_down, y, xg, xv, wg, wu, wd, acc, own, keep, sent, got, hid, rsent, rgot, yout,
           x_send, x_recv, x_load, wg_sem, wu_sem, wd_sem, p_send, p_recv, h_send, h_recv, r_send, r_recv, y_sem):
    dp, a, b = lax.axis_index("dp"), lax.axis_index("a"), lax.axis_index("b")
    nb = 4
    half = R // 2
    rows, xb = x.shape
    ff, dn = w_down.shape
    chunks, tiles = rows // R, ff // F
    steps = chunks * tiles
    third, sub = dn // GROUP, acc.shape[2]
    depth = F * GROUP
    down_groups = tiles // GROUP
    lag_sum = (2 * tiles) // 3
    mesh_id = pltpu.DeviceIdType.MESH if hasattr(pltpu, "DeviceIdType") else pl.DeviceIdType.MESH
    partner = (dp, 1 - a, b)

    def peer(o):
        return lax.rem(b + o, nb)

    def gather(c, o):
        r = pl.ds(pl.multiple_of(c * R, R), R)
        return pltpu.make_async_remote_copy(
            src_ref=x.at[r, :], dst_ref=xg.at[b, r, :], send_sem=x_send.at[c, o - 1], recv_sem=x_recv.at[c, o - 1],
            device_id=(dp, a, peer(o)), device_id_type=mesh_id)

    def loads(c):
        slot = lax.rem(c, 2)
        out = []
        for o in range(nb):
            for k in range(2):
                side = 1 - a if k == 0 else a
                r = pl.ds(pl.multiple_of(c * R + side * half, half), half)
                src = x.at[r, :] if o == 0 else xg.at[peer(o), r, :]
                cols = pl.ds(pl.multiple_of(peer(o) * xb, xb), xb)
                out.append(pltpu.make_async_copy(src, xv.at[slot, pl.ds(k * half, half), cols], x_load.at[o * 2 + k]))
        return out

    def weights(n):
        t = lax.rem(n, tiles)
        slot = lax.rem(n, WSLOTS)
        cols = pl.ds(pl.multiple_of(t * F, F), F)
        return (pltpu.make_async_copy(w_gate.at[:, cols], wg.at[slot], wg_sem.at[slot]),
                pltpu.make_async_copy(w_up.at[:, cols], wu.at[slot], wu_sem.at[slot]))

    def down_weights(q):
        slot = lax.rem(q, WSLOTS)
        j = lax.rem(q // GROUP, down_groups)
        i = lax.rem(q, GROUP)
        return pltpu.make_async_copy(
            w_down.at[pl.ds(pl.multiple_of(j * depth, depth), depth), pl.ds(pl.multiple_of(i * third, third), third)],
            wd.at[slot], wd_sem.at[slot])

    def partial(n):
        slot = lax.rem(n, SLOTS)
        return pltpu.make_async_remote_copy(
            src_ref=sent.at[slot], dst_ref=got.at[slot], send_sem=p_send.at[slot], recv_sem=p_recv.at[slot],
            device_id=partner, device_id_type=mesh_id)

    def hidden(m):
        slot = lax.rem(m // GROUP, HSLOTS)
        s = lax.rem(m, GROUP * HSLOTS)
        i = lax.rem(m, GROUP)
        cols = pl.ds(pl.multiple_of(i * F, F), F)
        return pltpu.make_async_remote_copy(
            src_ref=hid.at[slot, pl.ds(0, half), cols], dst_ref=hid.at[slot, pl.ds(half, half), cols],
            send_sem=h_send.at[s], recv_sem=h_recv.at[s], device_id=partner, device_id_type=mesh_id)

    def reduce(c, o):
        slot = lax.rem(c, 2)
        return pltpu.make_async_remote_copy(
            src_ref=rsent.at[o - 1], dst_ref=rgot.at[slot, o - 1], send_sem=r_send.at[o - 1],
            recv_sem=r_recv.at[slot, o - 1], device_id=(dp, a, peer(o)), device_id_type=mesh_id)

    def stores(c):
        out = []
        for k in range(2):
            side = a if k == 0 else 1 - a
            r = pl.ds(pl.multiple_of(c * R + side * half, half), half)
            out.append(pltpu.make_async_copy(yout.at[pl.ds(k * half, half), :], y.at[r, :], y_sem.at[k]))
        return out

    def finish(c):
        slot = lax.rem(c, 2)
        for o in range(1, nb):
            reduce(c, o).wait()

        @pl.when(c > 0)
        def _():
            for copy in stores(c - 1):
                copy.wait()

        for k in range(xb // sub):
            cols = pl.ds(k * sub, sub)
            total = own[k]
            for o in range(1, nb):
                total = total + rgot[slot, o - 1, :, cols].astype(jnp.float32)
            yout[:, cols] = total.astype(yout.dtype)
        for copy in stores(c):
            copy.start()

    barrier = pltpu.get_barrier_semaphore()
    for target in [partner] + [(dp, a, peer(o)) for o in range(1, nb)]:
        pl.semaphore_signal(barrier, inc=1, device_id=target, device_id_type=mesh_id)
    pl.semaphore_wait(barrier, nb)

    for o in (2, 3, 1):
        gather(0, o).start()
    for d in range(WSLOTS - 1):
        for copy in weights(d):
            copy.start()
    acc[...] = jnp.zeros_like(acc)
    for o in range(1, nb):
        gather(0, o).wait()
    for o in range(1, nb):
        if chunks > 1:
            gather(1, o).start()
    for copy in loads(0):
        copy.start()

    def step(n, _):
        c = n // tiles
        t = lax.rem(n, tiles)
        live = n < steps
        m = n - LAG_HIDDEN
        q = n - LAG_DOWN

        ahead = n + WSLOTS - 1

        @pl.when(ahead < steps)
        def _():
            for copy in weights(ahead):
                copy.start()

        @pl.when((ahead >= LAG_DOWN) & (ahead - LAG_DOWN < steps))
        def _():
            down_weights(ahead - LAG_DOWN).start()

        @pl.when(live & (t == 0))
        def _():
            for copy in loads(c):
                copy.wait()

        @pl.when(live & (t == 1) & (c + 2 < chunks))
        def _():
            for o in (2, 3, 1):
                gather(c + 2, o).start()

        @pl.when(live & (t == tiles // 2) & (c + 1 < chunks))
        def _():
            for o in range(1, nb):
                gather(c + 1, o).wait()
            for copy in loads(c + 1):
                copy.start()

        @pl.when((n >= SLOTS) & (n - SLOTS < steps))
        def _():
            partial(n - SLOTS).wait_send()

        @pl.when(live)
        def _():
            for copy in weights(n):
                copy.wait()
            slot = lax.rem(n, SLOTS)
            ws = lax.rem(n, WSLOTS)
            xs = lax.rem(c, 2)
            for k, w in enumerate((wg, wu)):
                v = jnp.dot(xv[xs], w[ws], preferred_element_type=jnp.float32)
                sent[slot, k] = v[:half].astype(sent.dtype)
                keep[slot, k] = v[half:]
            partial(n).start()

        old = m - GROUP * HSLOTS

        @pl.when((old >= 0) & (old < steps))
        def _():
            hidden(old).wait_send()

        @pl.when((m >= 0) & (m < steps))
        def _():
            partial(m).wait_recv()
            slot = lax.rem(m, SLOTS)
            g = keep[slot, 0] + got[slot, 0].astype(jnp.float32)
            u = keep[slot, 1] + got[slot, 1].astype(jnp.float32)
            cols = pl.ds(pl.multiple_of(lax.rem(m, GROUP) * F, F), F)
            hid[lax.rem(m // GROUP, HSLOTS), pl.ds(0, half), cols] = (jax.nn.silu(g) * u).astype(hid.dtype)
            hidden(m).start()

        @pl.when((q >= 0) & (q < steps))
        def _():
            i = lax.rem(q, GROUP)

            @pl.when(i == 0)
            def _():
                for d in range(GROUP):
                    hidden(q + d).wait_recv()

            down_weights(q).wait()
            hs = lax.rem(q // GROUP, HSLOTS)
            ws = lax.rem(q, WSLOTS)
            for k in range(third // sub):
                v = jnp.dot(hid[hs], wd[ws, :, pl.ds(k * sub, sub)], preferred_element_type=jnp.float32)
                at = i * (third // sub) + k
                acc[at] = acc[at] + v

            cq = q // tiles

            @pl.when(lax.rem(q, tiles) == tiles - 1)
            def _():
                per = xb // sub
                for o in (2, 3, 1):
                    for k in range(per):
                        rsent[o - 1, :, pl.ds(k * sub, sub)] = acc[peer(o) * per + k].astype(rsent.dtype)
                    reduce(cq, o).start()
                for k in range(per):
                    own[k] = acc[b * per + k]
                acc[...] = jnp.zeros_like(acc)

        late = q - lag_sum

        @pl.when((late >= 0) & (lax.rem(late, tiles) == tiles - 1) & (late < steps - 1))
        def _():
            finish(late // tiles)

        return 0

    lax.fori_loop(0, steps + LAG_HIDDEN + GROUP * HSLOTS, step, 0)
    finish(chunks - 1)
    for copy in stores(chunks - 1):
        copy.wait()


def mlp(x, w_gate, w_up, w_down):
    rows, xb = x.shape
    kd, ff = w_gate.shape
    dn = w_down.shape[1]
    sub = dn // 12
    third = dn // GROUP
    bf, f32 = jnp.bfloat16, jnp.float32
    chunks = rows // R
    dma = pltpu.SemaphoreType.DMA
    any_spec = pl.BlockSpec(memory_space=pl.ANY)
    out, _ = pl.pallas_call(
        kernel,
        out_shape=(jax.ShapeDtypeStruct((rows, xb), bf), jax.ShapeDtypeStruct((4, rows, xb), bf)),
        in_specs=[any_spec] * 4,
        out_specs=(any_spec, any_spec),
        scratch_shapes=[
            pltpu.VMEM((2, R, kd), bf),
            pltpu.VMEM((WSLOTS, kd, F), bf),
            pltpu.VMEM((WSLOTS, kd, F), bf),
            pltpu.VMEM((WSLOTS, F * GROUP, third), bf),
            pltpu.VMEM((12, R, sub), f32),
            pltpu.VMEM((xb // sub, R, sub), f32),
            pltpu.VMEM((SLOTS, 2, R // 2, F), f32),
            pltpu.VMEM((SLOTS, 2, R // 2, F), bf),
            pltpu.VMEM((SLOTS, 2, R // 2, F), bf),
            pltpu.VMEM((HSLOTS, R, F * GROUP), bf),
            pltpu.VMEM((3, R, xb), bf),
            pltpu.VMEM((2, 3, R, xb), bf),
            pltpu.VMEM((R, xb), bf),
            dma((chunks, 3)), dma((chunks, 3)), dma((8,)),
            dma((WSLOTS,)), dma((WSLOTS,)), dma((WSLOTS,)),
            dma((SLOTS,)), dma((SLOTS,)),
            dma((GROUP * HSLOTS,)), dma((GROUP * HSLOTS,)),
            dma((3,)), dma((2, 3)), dma((2,)),
        ],
        compiler_params=pltpu.CompilerParams(collective_id=0, has_side_effects=True, vmem_limit_bytes=VMEM_LIMIT),
        cost_estimate=pl.CostEstimate(flops=6 * rows * kd * ff, bytes_accessed=3 * chunks * kd * ff * 2,
                                      transcendentals=rows * ff),
    )(x, w_gate, w_up, w_down)
    return out


def solution(mesh):
    return jax.shard_map(mlp, mesh=mesh, in_specs=(P("dp", ("a", "b")), P("a", "b"), P("a", "b"), P("b", "a")),
                         out_specs=P("dp", ("a", "b")), check_vma=False)
```

```python
import functools
import jax
import jax.numpy as jnp
from jax import lax
from jax.experimental import pallas as pl
from jax.experimental.pallas import tpu as pltpu
from jax.sharding import PartitionSpec as P

R = 256
F = 256
GROUP = 3
LAG_HIDDEN = 4
LAG_DOWN = 12
SLOTS = LAG_DOWN + 2
HSLOTS = LAG_DOWN // GROUP + 1
WSLOTS = 3
VMEM_LIMIT = 66 * 1000 * 1000


def kernel(x, w_gate, w_up, w_down, y, xg, xv, wg, wu, wd, acc, own, keep, sent, got, hid, rsent, rgot, yout,
           x_send, x_recv, x_load, wg_sem, wu_sem, wd_sem, p_send, p_recv, h_send, h_recv, r_send, r_recv, y_sem):
    dp, a, b = lax.axis_index("dp"), lax.axis_index("a"), lax.axis_index("b")
    nb = 4
    half = R // 2
    rows, xb = x.shape
    ff, dn = w_down.shape
    chunks, tiles = rows // R, ff // F
    steps = chunks * tiles
    third, sub = dn // GROUP, acc.shape[2]
    per = xb // sub
    places = third // sub
    depth = F * GROUP
    down_groups = tiles // GROUP
    lag_sum = tiles // 2
    mesh_id = pltpu.DeviceIdType.MESH if hasattr(pltpu, "DeviceIdType") else pl.DeviceIdType.MESH
    partner = (dp, 1 - a, b)

    sibling = b + 1 - 2 * lax.rem(b, 2)
    across = lax.rem(b + 2, nb)
    diagonal = lax.rem(sibling + 2, nb)
    owners = (b, sibling, across, diagonal)

    def half_rows(c, k):
        side = 1 - a if k == 0 else a
        return pl.ds(pl.multiple_of(c * R + side * half, half), half)

    def gather(c, kind, k):
        r = half_rows(c, k)
        owner = across if kind == 2 else b
        return pltpu.make_async_remote_copy(
            src_ref=xg.at[owner, r, :] if kind == 2 else x.at[r, :], dst_ref=xg.at[owner, r, :],
            send_sem=x_send.at[c, kind, k], recv_sem=x_recv.at[c, kind, k],
            device_id=(dp, a, across if kind == 1 else sibling), device_id_type=mesh_id)

    def first(kind, k):
        owner = across if kind == 2 else b
        cols = pl.ds(pl.multiple_of(owner * xb, xb), xb)
        dst = xv.at[0, pl.ds(k * half, half), cols]
        return pltpu.make_async_remote_copy(
            src_ref=dst if kind == 2 else x.at[half_rows(0, k), :], dst_ref=dst,
            send_sem=x_send.at[0, kind, k], recv_sem=x_recv.at[0, kind, k],
            device_id=(dp, a, across if kind == 1 else sibling), device_id_type=mesh_id)

    def load(c, o, k):
        r = half_rows(c, k)
        src = x.at[r, :] if o == 0 else xg.at[owners[o], r, :]
        cols = pl.ds(pl.multiple_of(owners[o] * xb, xb), xb)
        return pltpu.make_async_copy(src, xv.at[lax.rem(c, 2), pl.ds(k * half, half), cols], x_load.at[o, k])

    def weights(n):
        t = lax.rem(n, tiles)
        slot = lax.rem(n, WSLOTS)
        cols = pl.ds(pl.multiple_of(t * F, F), F)
        return (pltpu.make_async_copy(w_gate.at[:, cols], wg.at[slot], wg_sem.at[slot]),
                pltpu.make_async_copy(w_up.at[:, cols], wu.at[slot], wu_sem.at[slot]))

    def owner_at(p):
        e = p // per
        return 2 * lax.rem(b // 2 + 1 - e // 2, 2) + lax.rem(lax.rem(b, 2) + 1 - lax.rem(e, 2), 2)

    def down_weights(q, slot):
        j = lax.rem(q // GROUP, down_groups)
        i = lax.rem(q, GROUP)
        r = pl.ds(pl.multiple_of(j * depth, depth), depth)
        out = []
        for k in range(places):
            p = i * places + k
            at = owner_at(p) * per + lax.rem(p, per)
            out.append(pltpu.make_async_copy(
                w_down.at[r, pl.ds(pl.multiple_of(at * sub, sub), sub)], wd.at[slot, k], wd_sem.at[slot, k]))
        return out

    def partial(n):
        slot = lax.rem(n, SLOTS)
        return pltpu.make_async_remote_copy(
            src_ref=sent.at[slot], dst_ref=got.at[slot], send_sem=p_send.at[slot], recv_sem=p_recv.at[slot],
            device_id=partner, device_id_type=mesh_id)

    def hidden(m):
        slot = lax.rem(m // GROUP, HSLOTS)
        s = lax.rem(m, GROUP * HSLOTS)
        i = lax.rem(m, GROUP)
        cols = pl.ds(pl.multiple_of(i * F, F), F)
        return pltpu.make_async_remote_copy(
            src_ref=hid.at[slot, pl.ds(0, half), cols], dst_ref=hid.at[slot, pl.ds(half, half), cols],
            send_sem=h_send.at[s], recv_sem=h_recv.at[s], device_id=partner, device_id_type=mesh_id)

    own_rows, partner_rows, all_rows = pl.ds(0, half), pl.ds(half, half), pl.ds(0, R)

    def reduce(c, kind, k, r=all_rows, s=0):
        slot = lax.rem(c, 2)
        return pltpu.make_async_remote_copy(
            src_ref=rsent.at[kind, k, r], dst_ref=rgot.at[slot, kind, k, r], send_sem=r_send.at[kind, k, s],
            recv_sem=r_recv.at[slot, kind, k, s], device_id=(dp, a, across if kind == 2 else sibling),
            device_id_type=mesh_id)

    def stores(c, k, sides=(0, 1)):
        cols = pl.ds(k * sub, sub)
        return [pltpu.make_async_copy(yout.at[pl.ds(s * half, half), cols], y.at[half_rows(c, 1 - s), cols],
                                      y_sem.at[s, k]) for s in sides]

    def combine(c, third_done, r=all_rows, s=0):
        slot = lax.rem(c, 2)
        for k in range(per):
            if third_done == 0:
                rsent[0, k, r] = acc[k, r].astype(rsent.dtype)
                reduce(c, 0, k, r, s).start()
            elif third_done == 1:
                reduce(c, 0, k, r, s).wait_recv()
                total = acc[per + k, r] + rgot[slot, 0, k, r].astype(jnp.float32)
                rsent[2, k, r] = total.astype(rsent.dtype)
                reduce(c, 2, k, r, s).start()
            else:
                rsent[1, k, r] = acc[2 * per + k, r].astype(rsent.dtype)
                reduce(c, 1, k, r, s).start()
                own[k, r] = acc[3 * per + k, r]

    def stored(c):
        for k in range(per):
            for copy in stores(c, k):
                copy.wait()

    def finish(c, r=all_rows, s=0, sides=(0, 1)):
        slot = lax.rem(c, 2)
        for k in range(per):
            reduce(c, 1, k, r, s).wait_recv()
            reduce(c, 2, k, r, s).wait_recv()
            total = own[k, r] + rgot[slot, 1, k, r].astype(jnp.float32) + rgot[slot, 2, k, r].astype(jnp.float32)
            yout[r, pl.ds(k * sub, sub)] = total.astype(yout.dtype)
            for copy in stores(c, k, sides):
                copy.start()
        for k in range(per):
            for kind in range(3):
                reduce(c, kind, k, r, s).wait_send()

    def activate(m):
        partial(m).wait_recv()
        slot = lax.rem(m, SLOTS)
        g = keep[slot, 0] + got[slot, 0].astype(jnp.float32)
        u = keep[slot, 1] + got[slot, 1].astype(jnp.float32)
        cols = pl.ds(pl.multiple_of(lax.rem(m, GROUP) * F, F), F)
        hid[lax.rem(m // GROUP, HSLOTS), pl.ds(0, half), cols] = (jax.nn.silu(g) * u).astype(hid.dtype)
        hidden(m).start()

    def down(q, ws, r=all_rows):
        i = lax.rem(q, GROUP)
        for copy in down_weights(q, ws):
            copy.wait()
        hs = lax.rem(q // GROUP, HSLOTS)
        for k in range(places):
            v = jnp.dot(hid[hs, r], wd[ws, k], preferred_element_type=jnp.float32)
            at = i * places + k
            acc[at, r] = acc[at, r] + v

    barrier = pltpu.get_barrier_semaphore()
    for target in (partner, (dp, a, sibling), (dp, a, across)):
        pl.semaphore_signal(barrier, inc=1, device_id=target, device_id_type=mesh_id)
    pl.semaphore_wait(barrier, 3)

    for k in range(2):
        first(1, k).start()
        first(0, k).start()
        load(0, 0, k).start()
    for d in range(WSLOTS):
        for copy in weights(d):
            copy.start()
    acc[...] = jnp.zeros_like(acc)
    for k in range(2):
        first(1, k).wait_recv()
        first(2, k).start()
        first(0, k).wait_recv()
        load(0, 0, k).wait()
        first(2, k).wait_recv()
        if k == 0:
            for d in range(WSLOTS):
                for copy in weights(d):
                    copy.wait()
                for i, w in enumerate((wg, wu)):
                    sent[d, i] = jnp.dot(xv[0, :half], w[d], preferred_element_type=jnp.float32).astype(sent.dtype)
                partial(d).start()
    for k in range(2):
        for kind in range(3):
            first(kind, k).wait_send()
    for k in range(2):
        for kind in (1, 0):
            if chunks > 1:
                gather(1, kind, k).start()

    def step(n, _):
        c = n // tiles
        t = lax.rem(n, tiles)
        m = n - LAG_HIDDEN
        q = n - LAG_DOWN

        ahead = n + WSLOTS - 1

        @pl.when((ahead >= WSLOTS) & (ahead < steps))
        def _():
            for copy in weights(ahead):
                copy.start()

        @pl.when((ahead >= LAG_DOWN) & (ahead < steps + 2))
        def _():
            for copy in down_weights(ahead - LAG_DOWN, lax.rem(ahead - LAG_DOWN, WSLOTS)):
                copy.start()

        @pl.when((t == 0) & (c > 0))
        def _():
            for o in range(nb):
                for k in range(2):
                    load(c, o, k).wait()

        @pl.when((t == 1) & (c + 2 < chunks))
        def _():
            for k in range(2):
                for kind in (1, 0):
                    gather(c + 2, kind, k).start()

        @pl.when((t == tiles // 3) & (c + 1 < chunks))
        def _():
            for k in range(2):
                gather(c + 1, 1, k).wait_recv()
                gather(c + 1, 2, k).start()

        @pl.when((t == 2 * tiles // 3) & (c + 1 < chunks))
        def _():
            for k in range(2):
                gather(c + 1, 0, k).wait_recv()
                gather(c + 1, 2, k).wait_recv()
                for o in range(nb):
                    load(c + 1, o, k).start()
                for kind in range(3):
                    gather(c + 1, kind, k).wait_send()

        @pl.when(n >= SLOTS)
        def _():
            partial(n - SLOTS).wait_send()

        @pl.when(n < WSLOTS)
        def _():
            for k, w in enumerate((wg, wu)):
                keep[n, k] = jnp.dot(xv[0, half:], w[n], preferred_element_type=jnp.float32)

        @pl.when(n >= WSLOTS)
        def _():
            for copy in weights(n):
                copy.wait()
            slot = lax.rem(n, SLOTS)
            ws = lax.rem(n, WSLOTS)
            xs = lax.rem(c, 2)
            for k, w in enumerate((wg, wu)):
                v = jnp.dot(xv[xs], w[ws], preferred_element_type=jnp.float32)
                sent[slot, k] = v[:half].astype(sent.dtype)
                keep[slot, k] = v[half:]
            partial(n).start()

        old = m - GROUP * HSLOTS

        @pl.when(old >= 0)
        def _():
            hidden(old).wait_send()

        @pl.when(m >= 0)
        def _():
            activate(m)

        @pl.when(q >= 0)
        def _():
            @pl.when(lax.rem(q, GROUP) == 0)
            def _():
                for d in range(GROUP):
                    hidden(q + d).wait_recv()

            down(q, lax.rem(q, WSLOTS))
            cq, tq = q // tiles, lax.rem(q, tiles)
            for i in range(GROUP):
                @pl.when(tq == tiles - GROUP + i)
                def _():
                    combine(cq, i)
                    if i == GROUP - 1:
                        acc[...] = jnp.zeros_like(acc)

        late = q - lag_sum

        @pl.when((late >= 0) & (lax.rem(late, tiles) == tiles - 1))
        def _():
            @pl.when(late // tiles > 0)
            def _():
                stored(late // tiles - 1)

            finish(late // tiles)

        return 0

    lax.fori_loop(0, steps, step, 0)

    last = chunks - 1
    stored(last - 1)
    end = [(q, all_rows) for q in range(steps - 12, steps - 6)]
    end += [(q, own_rows) for q in range(steps - 6, steps)] + [(q, partner_rows) for q in range(steps - 6, steps)]
    for e, (q, r) in enumerate(end):
        if e % GROUP == 0 and e // GROUP < LAG_HIDDEN:
            m = steps - LAG_HIDDEN + e // GROUP
            hidden(m - GROUP * HSLOTS).wait_send()
            activate(m)
        if e + 2 < len(end):
            for copy in down_weights(end[e + 2][0], (steps - 12 + e + 2) % WSLOTS):
                copy.start()
        if q % GROUP == 0 and r is not own_rows:
            for d in range(GROUP):
                hidden(q + d).wait_recv()
        down(q, (steps - 12 + e) % WSLOTS, r)
        if q >= steps - GROUP:
            combine(last, q % GROUP, r, 0 if r is own_rows else 1)
    finish(last, own_rows, 0, (0,))
    finish(last, partner_rows, 1, (1,))
    for d in range(SLOTS):
        partial(steps - SLOTS + d).wait_send()
    for d in range(GROUP * HSLOTS):
        hidden(steps - GROUP * HSLOTS + d).wait_send()
    stored(last)


def mlp(x, w_gate, w_up, w_down):
    rows, xb = x.shape
    kd, ff = w_gate.shape
    dn = w_down.shape[1]
    sub = dn // 12
    third = dn // GROUP
    bf, f32 = jnp.bfloat16, jnp.float32
    chunks = rows // R
    dma = pltpu.SemaphoreType.DMA
    any_spec = pl.BlockSpec(memory_space=pl.ANY)
    out, _ = pl.pallas_call(
        kernel,
        out_shape=(jax.ShapeDtypeStruct((rows, xb), bf), jax.ShapeDtypeStruct((4, rows, xb), bf)),
        in_specs=[any_spec] * 4,
        out_specs=(any_spec, any_spec),
        scratch_shapes=[
            pltpu.VMEM((2, R, kd), bf),
            pltpu.VMEM((WSLOTS, kd, F), bf),
            pltpu.VMEM((WSLOTS, kd, F), bf),
            pltpu.VMEM((WSLOTS, third // sub, F * GROUP, sub), bf),
            pltpu.VMEM((12, R, sub), f32),
            pltpu.VMEM((xb // sub, R, sub), f32),
            pltpu.VMEM((SLOTS, 2, R // 2, F), f32),
            pltpu.VMEM((SLOTS, 2, R // 2, F), bf),
            pltpu.VMEM((SLOTS, 2, R // 2, F), bf),
            pltpu.VMEM((HSLOTS, R, F * GROUP), bf),
            pltpu.VMEM((3, xb // sub, R, sub), bf),
            pltpu.VMEM((2, 3, xb // sub, R, sub), bf),
            pltpu.VMEM((R, xb), bf),
            dma((chunks, 3, 2)), dma((chunks, 3, 2)), dma((4, 2)),
            dma((WSLOTS,)), dma((WSLOTS,)), dma((WSLOTS, third // sub)),
            dma((SLOTS,)), dma((SLOTS,)),
            dma((GROUP * HSLOTS,)), dma((GROUP * HSLOTS,)),
            dma((3, xb // sub, 2)), dma((2, 3, xb // sub, 2)), dma((2, xb // sub)),
        ],
        compiler_params=pltpu.CompilerParams(collective_id=0, has_side_effects=True, vmem_limit_bytes=VMEM_LIMIT),
        cost_estimate=pl.CostEstimate(flops=6 * rows * kd * ff, bytes_accessed=3 * chunks * kd * ff * 2,
                                      transcendentals=rows * ff),
    )(x, w_gate, w_up, w_down)
    return out


def solution(mesh):
    return jax.shard_map(mlp, mesh=mesh, in_specs=(P("dp", ("a", "b")), P("a", "b"), P("a", "b"), P("b", "a")),
                         out_specs=P("dp", ("a", "b")), check_vma=False)
```

```python
import functools
import jax
import jax.numpy as jnp
from jax import lax
from jax.experimental import pallas as pl
from jax.experimental.pallas import tpu as pltpu
from jax.sharding import PartitionSpec as P

R = 256
F = 256
GROUP = 3
LAG_HIDDEN = 4
LAG_DOWN = 12
SLOTS = LAG_DOWN + 2
HSLOTS = LAG_DOWN // GROUP + 1
WSLOTS = 3
VMEM_LIMIT = 66 * 1000 * 1000


def kernel(x, w_gate, w_up, w_down, y, xg, xv, wg, wu, wd, acc, own, keep, sent, got, hid, rsent, rgot, yout,
           x_send, x_recv, x_load, wg_sem, wu_sem, wd_sem, p_send, p_recv, h_send, h_recv, r_send, r_recv, y_sem):
    dp, a, b = lax.axis_index("dp"), lax.axis_index("a"), lax.axis_index("b")
    nb = 4
    half = R // 2
    rows, xb = x.shape
    ff, dn = w_down.shape
    chunks, tiles = rows // R, ff // F
    steps = chunks * tiles
    third, sub = dn // GROUP, acc.shape[2]
    per = xb // sub
    places = third // sub
    depth = F * GROUP
    down_groups = tiles // GROUP
    lag_sum = tiles // 2
    mesh_id = pltpu.DeviceIdType.MESH if hasattr(pltpu, "DeviceIdType") else pl.DeviceIdType.MESH
    partner = (dp, 1 - a, b)

    sibling = b + 1 - 2 * lax.rem(b, 2)
    across = lax.rem(b + 2, nb)
    diagonal = lax.rem(sibling + 2, nb)
    owners = (b, sibling, across, diagonal)

    def half_rows(c, k):
        side = 1 - a if k == 0 else a
        return pl.ds(pl.multiple_of(c * R + side * half, half), half)

    def gather(c, kind, k):
        r = half_rows(c, k)
        owner = across if kind == 2 else b
        return pltpu.make_async_remote_copy(
            src_ref=xg.at[owner, r, :] if kind == 2 else x.at[r, :], dst_ref=xg.at[owner, r, :],
            send_sem=x_send.at[c, kind, k], recv_sem=x_recv.at[c, kind, k],
            device_id=(dp, a, across if kind == 1 else sibling), device_id_type=mesh_id)

    def first(kind, k):
        owner = across if kind == 2 else b
        cols = pl.ds(pl.multiple_of(owner * xb, xb), xb)
        dst = xv.at[0, pl.ds(k * half, half), cols]
        return pltpu.make_async_remote_copy(
            src_ref=dst if kind == 2 else x.at[half_rows(0, k), :], dst_ref=dst,
            send_sem=x_send.at[0, kind, k], recv_sem=x_recv.at[0, kind, k],
            device_id=(dp, a, across if kind == 1 else sibling), device_id_type=mesh_id)

    def load(c, o, k):
        r = half_rows(c, k)
        src = x.at[r, :] if o == 0 else xg.at[owners[o], r, :]
        cols = pl.ds(pl.multiple_of(owners[o] * xb, xb), xb)
        return pltpu.make_async_copy(src, xv.at[lax.rem(c, 2), pl.ds(k * half, half), cols], x_load.at[o, k])

    def weights(n, slot):
        t = lax.rem(n, tiles)
        cols = pl.ds(pl.multiple_of(t * F, F), F)
        return (pltpu.make_async_copy(w_gate.at[:, cols], wg.at[slot], wg_sem.at[slot]),
                pltpu.make_async_copy(w_up.at[:, cols], wu.at[slot], wu_sem.at[slot]))

    def owner_at(p):
        e = p // per
        return 2 * lax.rem(b // 2 + 1 - e // 2, 2) + lax.rem(lax.rem(b, 2) + 1 - lax.rem(e, 2), 2)

    def down_weights(q, slot):
        j = lax.rem(q // GROUP, down_groups)
        i = lax.rem(q, GROUP)
        r = pl.ds(pl.multiple_of(j * depth, depth), depth)
        out = []
        for k in range(places):
            p = i * places + k
            at = owner_at(p) * per + lax.rem(p, per)
            out.append(pltpu.make_async_copy(
                w_down.at[r, pl.ds(pl.multiple_of(at * sub, sub), sub)], wd.at[slot, k], wd_sem.at[slot, k]))
        return out

    def partial(n):
        slot = lax.rem(n, SLOTS)
        return pltpu.make_async_remote_copy(
            src_ref=sent.at[slot], dst_ref=got.at[slot], send_sem=p_send.at[slot], recv_sem=p_recv.at[slot],
            device_id=partner, device_id_type=mesh_id)

    def send_and_keep(n, ws, xs):
        for copy in weights(n, ws):
            copy.wait()
        slot = lax.rem(n, SLOTS)
        for k, w in enumerate((wg, wu)):
            v = jnp.dot(xv[xs], w[ws], preferred_element_type=jnp.float32)
            sent[slot, k] = v[:half].astype(sent.dtype)
            keep[slot, k] = v[half:]
        partial(n).start()

    def hidden(m):
        slot = lax.rem(m // GROUP, HSLOTS)
        s = lax.rem(m, GROUP * HSLOTS)
        i = lax.rem(m, GROUP)
        cols = pl.ds(pl.multiple_of(i * F, F), F)
        return pltpu.make_async_remote_copy(
            src_ref=hid.at[slot, pl.ds(0, half), cols], dst_ref=hid.at[slot, pl.ds(half, half), cols],
            send_sem=h_send.at[s], recv_sem=h_recv.at[s], device_id=partner, device_id_type=mesh_id)

    own_rows, partner_rows, all_rows = pl.ds(0, half), pl.ds(half, half), pl.ds(0, R)

    def reduce(c, kind, k, r=all_rows, s=0):
        slot = lax.rem(c, 2)
        return pltpu.make_async_remote_copy(
            src_ref=rsent.at[kind, k, r], dst_ref=rgot.at[slot, kind, k, r], send_sem=r_send.at[kind, k, s],
            recv_sem=r_recv.at[slot, kind, k, s], device_id=(dp, a, across if kind == 2 else sibling),
            device_id_type=mesh_id)

    def stores(c, k, sides=(0, 1)):
        cols = pl.ds(k * sub, sub)
        return [pltpu.make_async_copy(yout.at[pl.ds(s * half, half), cols], y.at[half_rows(c, 1 - s), cols],
                                      y_sem.at[s, k]) for s in sides]

    def combine(c, third_done, r=all_rows, s=0):
        slot = lax.rem(c, 2)
        for k in range(per):
            if third_done == 0:
                rsent[0, k, r] = acc[k, r].astype(rsent.dtype)
                reduce(c, 0, k, r, s).start()
            elif third_done == 1:
                reduce(c, 0, k, r, s).wait_recv()
                total = acc[per + k, r] + rgot[slot, 0, k, r].astype(jnp.float32)
                rsent[2, k, r] = total.astype(rsent.dtype)
                reduce(c, 2, k, r, s).start()
            else:
                rsent[1, k, r] = acc[2 * per + k, r].astype(rsent.dtype)
                reduce(c, 1, k, r, s).start()
                own[k, r] = acc[3 * per + k, r]

    def stored(c):
        for k in range(per):
            for copy in stores(c, k):
                copy.wait()

    def finish(c, r=all_rows, s=0, sides=(0, 1)):
        slot = lax.rem(c, 2)
        for k in range(per):
            reduce(c, 1, k, r, s).wait_recv()
            reduce(c, 2, k, r, s).wait_recv()
            total = own[k, r] + rgot[slot, 1, k, r].astype(jnp.float32) + rgot[slot, 2, k, r].astype(jnp.float32)
            yout[r, pl.ds(k * sub, sub)] = total.astype(yout.dtype)
            for copy in stores(c, k, sides):
                copy.start()
        for k in range(per):
            for kind in range(3):
                reduce(c, kind, k, r, s).wait_send()

    def activate(m):
        partial(m).wait_recv()
        slot = lax.rem(m, SLOTS)
        g = keep[slot, 0] + got[slot, 0].astype(jnp.float32)
        u = keep[slot, 1] + got[slot, 1].astype(jnp.float32)
        cols = pl.ds(pl.multiple_of(lax.rem(m, GROUP) * F, F), F)
        hid[lax.rem(m // GROUP, HSLOTS), pl.ds(0, half), cols] = (jax.nn.silu(g) * u).astype(hid.dtype)
        hidden(m).start()

    def down(q, ws, r=all_rows):
        i = lax.rem(q, GROUP)
        for copy in down_weights(q, ws):
            copy.wait()
        hs = lax.rem(q // GROUP, HSLOTS)
        for k in range(places):
            v = jnp.dot(hid[hs, r], wd[ws, k], preferred_element_type=jnp.float32)
            at = i * places + k
            acc[at, r] = acc[at, r] + v

    barrier = pltpu.get_barrier_semaphore()
    for target in (partner, (dp, a, sibling), (dp, a, across)):
        pl.semaphore_signal(barrier, inc=1, device_id=target, device_id_type=mesh_id)
    pl.semaphore_wait(barrier, 3)

    for k in range(2):
        first(1, k).start()
        first(0, k).start()
        load(0, 0, k).start()
    for d in range(WSLOTS):
        for copy in weights(d, d):
            copy.start()
    acc[...] = jnp.zeros_like(acc)

    start_steps = [d for d in range(WSLOTS)]
    for d in range(WSLOTS):
        start_steps += [WSLOTS + d, d]

    def fetch(e):
        n = start_steps[e] if e < len(start_steps) else e - WSLOTS
        for copy in weights(n, e % WSLOTS):
            copy.start()

    for k in range(2):
        first(1, k).wait_recv()
        first(2, k).start()
        first(0, k).wait_recv()
        load(0, 0, k).wait()
        first(2, k).wait_recv()
        if k == 0:
            for d in range(WSLOTS):
                for copy in weights(d, d):
                    copy.wait()
                for i, w in enumerate((wg, wu)):
                    sent[d, i] = jnp.dot(xv[0, :half], w[d], preferred_element_type=jnp.float32).astype(sent.dtype)
                partial(d).start()
                fetch(WSLOTS + d)
    for k in range(2):
        for kind in range(3):
            first(kind, k).wait_send()
    for k in range(2):
        for kind in (1, 0):
            if chunks > 1:
                gather(1, kind, k).start()

    for e in range(WSLOTS, len(start_steps)):
        n = start_steps[e]
        if e > WSLOTS:
            fetch(e + WSLOTS - 1)
        if n >= WSLOTS:
            send_and_keep(n, e % WSLOTS, 0)
        else:
            for copy in weights(n, e % WSLOTS):
                copy.wait()
            for k, w in enumerate((wg, wu)):
                keep[n, k] = jnp.dot(xv[0, half:], w[e % WSLOTS], preferred_element_type=jnp.float32)
            m = n + WSLOTS - LAG_HIDDEN
            if m >= 0:
                activate(m)
    for k in range(2):
        for kind in (1, 0):
            if chunks > 2:
                gather(2, kind, k).start()

    def step(n, _):
        c = n // tiles
        t = lax.rem(n, tiles)
        m = n - LAG_HIDDEN
        q = n - LAG_DOWN

        ahead = n + WSLOTS - 1

        @pl.when(ahead < steps)
        def _():
            for copy in weights(ahead, lax.rem(ahead, WSLOTS)):
                copy.start()

        @pl.when((ahead >= LAG_DOWN) & (ahead < steps + 2))
        def _():
            for copy in down_weights(ahead - LAG_DOWN, lax.rem(ahead - LAG_DOWN, WSLOTS)):
                copy.start()

        @pl.when((t == 0) & (c > 0))
        def _():
            for o in range(nb):
                for k in range(2):
                    load(c, o, k).wait()

        @pl.when((t == 1) & (c + 2 < chunks))
        def _():
            for k in range(2):
                for kind in (1, 0):
                    gather(c + 2, kind, k).start()

        @pl.when((t == tiles // 3) & (c + 1 < chunks))
        def _():
            for k in range(2):
                gather(c + 1, 1, k).wait_recv()
                gather(c + 1, 2, k).start()

        @pl.when((t == 2 * tiles // 3) & (c + 1 < chunks))
        def _():
            for k in range(2):
                gather(c + 1, 0, k).wait_recv()
                gather(c + 1, 2, k).wait_recv()
                for o in range(nb):
                    load(c + 1, o, k).start()
                for kind in range(3):
                    gather(c + 1, kind, k).wait_send()

        @pl.when(n >= SLOTS)
        def _():
            partial(n - SLOTS).wait_send()

        send_and_keep(n, lax.rem(n, WSLOTS), lax.rem(c, 2))

        old = m - GROUP * HSLOTS

        @pl.when(old >= 0)
        def _():
            hidden(old).wait_send()

        activate(m)

        @pl.when(q >= 0)
        def _():
            @pl.when(lax.rem(q, GROUP) == 0)
            def _():
                for d in range(GROUP):
                    hidden(q + d).wait_recv()

            down(q, lax.rem(q, WSLOTS))
            cq, tq = q // tiles, lax.rem(q, tiles)
            for i in range(GROUP):
                @pl.when(tq == tiles - GROUP + i)
                def _():
                    combine(cq, i)
                    if i == GROUP - 1:
                        acc[...] = jnp.zeros_like(acc)

        late = q - lag_sum

        @pl.when((late >= 0) & (lax.rem(late, tiles) == tiles - 1))
        def _():
            @pl.when(late // tiles > 0)
            def _():
                stored(late // tiles - 1)

            finish(late // tiles)

        return 0

    lax.fori_loop(2 * WSLOTS, steps, step, 0)

    last = chunks - 1
    stored(last - 1)
    end = [(q, all_rows) for q in range(steps - 12, steps - 6)]
    end += [(q, own_rows) for q in range(steps - 6, steps)] + [(q, partner_rows) for q in range(steps - 6, steps)]
    for e, (q, r) in enumerate(end):
        if e % GROUP == 0 and e // GROUP < LAG_HIDDEN:
            m = steps - LAG_HIDDEN + e // GROUP
            hidden(m - GROUP * HSLOTS).wait_send()
            activate(m)
        if e + 2 < len(end):
            for copy in down_weights(end[e + 2][0], (steps - 12 + e + 2) % WSLOTS):
                copy.start()
        if q % GROUP == 0 and r is not own_rows:
            for d in range(GROUP):
                hidden(q + d).wait_recv()
        down(q, (steps - 12 + e) % WSLOTS, r)
        if q >= steps - GROUP:
            combine(last, q % GROUP, r, 0 if r is own_rows else 1)
    finish(last, own_rows, 0, (0,))
    finish(last, partner_rows, 1, (1,))
    for d in range(SLOTS):
        partial(steps - SLOTS + d).wait_send()
    for d in range(GROUP * HSLOTS):
        hidden(steps - GROUP * HSLOTS + d).wait_send()
    stored(last)


def mlp(x, w_gate, w_up, w_down):
    rows, xb = x.shape
    kd, ff = w_gate.shape
    dn = w_down.shape[1]
    sub = dn // 12
    third = dn // GROUP
    bf, f32 = jnp.bfloat16, jnp.float32
    chunks = rows // R
    dma = pltpu.SemaphoreType.DMA
    any_spec = pl.BlockSpec(memory_space=pl.ANY)
    out, _ = pl.pallas_call(
        kernel,
        out_shape=(jax.ShapeDtypeStruct((rows, xb), bf), jax.ShapeDtypeStruct((4, rows, xb), bf)),
        in_specs=[any_spec] * 4,
        out_specs=(any_spec, any_spec),
        scratch_shapes=[
            pltpu.VMEM((2, R, kd), bf),
            pltpu.VMEM((WSLOTS, kd, F), bf),
            pltpu.VMEM((WSLOTS, kd, F), bf),
            pltpu.VMEM((WSLOTS, third // sub, F * GROUP, sub), bf),
            pltpu.VMEM((12, R, sub), f32),
            pltpu.VMEM((xb // sub, R, sub), f32),
            pltpu.VMEM((SLOTS, 2, R // 2, F), f32),
            pltpu.VMEM((SLOTS, 2, R // 2, F), bf),
            pltpu.VMEM((SLOTS, 2, R // 2, F), bf),
            pltpu.VMEM((HSLOTS, R, F * GROUP), bf),
            pltpu.VMEM((3, xb // sub, R, sub), bf),
            pltpu.VMEM((2, 3, xb // sub, R, sub), bf),
            pltpu.VMEM((R, xb), bf),
            dma((chunks, 3, 2)), dma((chunks, 3, 2)), dma((4, 2)),
            dma((WSLOTS,)), dma((WSLOTS,)), dma((WSLOTS, third // sub)),
            dma((SLOTS,)), dma((SLOTS,)),
            dma((GROUP * HSLOTS,)), dma((GROUP * HSLOTS,)),
            dma((3, xb // sub, 2)), dma((2, 3, xb // sub, 2)), dma((2, xb // sub)),
        ],
        compiler_params=pltpu.CompilerParams(collective_id=0, has_side_effects=True, vmem_limit_bytes=VMEM_LIMIT),
        cost_estimate=pl.CostEstimate(flops=6 * rows * kd * ff, bytes_accessed=3 * chunks * kd * ff * 2,
                                      transcendentals=rows * ff),
    )(x, w_gate, w_up, w_down)
    return out


def solution(mesh):
    return jax.shard_map(mlp, mesh=mesh, in_specs=(P("dp", ("a", "b")), P("a", "b"), P("a", "b"), P("b", "a")),
                         out_specs=P("dp", ("a", "b")), check_vma=False)
```
